128 devices in a mesh: gx: 16 (over x, y), gy: 8 (over z, core).
Axes of the slice: x: 4, y: 4, z: 4, core: 2. Of those that a mesh axis runs over, the one named last changes fastest.
Arguments:
- ocean_heat_field: float32 [16, 384, 128, 128], P('gy', 'gx'), may hold values from -6 to 6
- patch_zone: int32 [384], replicated, may hold values from 0 to 127, as said below
- patch_position: int32 [384], replicated, may hold values from 0 to 5, as said below
- quarter_spins: int32 [384], replicated, may hold values from 0 to 3
- zone_patch_tally: int32 [128], P(('gx', 'gy')), may hold values from 0 to 6, as said below
Outputs:
- regional: float32 [16, 128, 6, 128, 128], P(None, ('gx', 'gy'))
The draws below stay inside these ranges and needn't reach their ends.
Inputs may be any that keep to these rules, and one draw needn't show every extreme that they name: In each aligned group of 24 blocks no more than 3 go to regions of one column patch_zone // 8, and each group has a column with exactly 3. A region receives at most 6 blocks and some region receives exactly 6. `patch_position`: the blocks of one region have distinct slots 0 to zone_patch_tally of that region minus 1, in increasing block order. zone_patch_tally[r] is the number of blocks j with patch_zone[j] = r.
All inputs are finite; a program needn't handle non-finite values.
Results may differ from the reference program's by a relative error of at most 0.00002.
Values sent between devices are 32-bit elements; how exact they have to be, the bound alone decides.
A program may use at most 128 MiB of HBM per device.

```python
import jax
import jax.numpy as jnp

PATCH_SIDE = 128
BLK_DEV = 24
INPUT_PATCHES = 384
EPOCH_TOTAL = 16
REGIONS = 128
MOST = 3
CAP = 6


def rank_within(labels, label_count):
    onehot = (labels[:, None] == jnp.arange(label_count, dtype=jnp.int32)[None, :]).astype(jnp.int32)
    running = jnp.cumsum(onehot, axis=0) - onehot
    return jnp.sum(running * onehot, axis=1).astype(jnp.int32)


def routing(key):
    column_count = INPUT_PATCHES // BLK_DEV
    row_count = REGIONS // column_count
    column_slots = column_count * MOST
    group_key = jax.random.fold_in(key, 101)
    order_key = jax.random.fold_in(key, 202)

    def group_columns(subkey):
        pick_key, score_key, shuffle_key = jax.random.split(subkey, 3)
        chosen = jax.random.randint(pick_key, (), 0, column_count, dtype=jnp.int32)
        slot_ids = jnp.arange(column_slots, dtype=jnp.int32)
        scores = jax.random.permutation(score_key, column_slots).astype(jnp.int32)
        scores = jnp.where(slot_ids // MOST == chosen, slot_ids % MOST - MOST, scores)
        ranked = jnp.argsort(scores, stable=True).astype(jnp.int32)
        return jax.random.permutation(shuffle_key, ranked[:BLK_DEV] // MOST)
    columns = jax.vmap(group_columns)(jax.random.split(group_key, column_count)).reshape(-1)

    def column_order(subkey):
        pick_key, score_key = jax.random.split(subkey)
        chosen = jax.random.randint(pick_key, (), 0, row_count, dtype=jnp.int32)
        slot_ids = jnp.arange(column_slots, dtype=jnp.int32)
        scores = jax.random.permutation(score_key, column_slots).astype(jnp.int32)
        scores = jnp.where(slot_ids // CAP == chosen, slot_ids % CAP - CAP, scores)
        return jnp.argsort(scores, stable=True).astype(jnp.int32)
    orders = jax.vmap(column_order)(jax.random.split(order_key, column_count))
    within = rank_within(columns, column_count)
    rows = orders[columns, within] // CAP
    regions = (columns * row_count + rows).astype(jnp.int32)
    slots = rank_within(regions, REGIONS)
    counts = jnp.sum((regions[:, None] == jnp.arange(REGIONS, dtype=jnp.int32)[None, :]).astype(jnp.int32), axis=0)
    return (regions, slots, counts.astype(jnp.int32))


def draw_patch_zone(key, part):
    return routing(key)[0]


def draw_patch_position(key, part):
    return routing(key)[1]


def draw_zone_patch_tally(key, part):
    return routing(key)[2]


def plant(array, key, smallest, largest):
    shape = array.shape
    index_at = [jax.random.randint(jax.random.fold_in(key, axis), (), 0, shape[axis]) for axis in range(len(shape))]
    array = array.at[tuple(index_at)].set(smallest)
    longest = shape.index(max(shape))
    index_at[longest] = (index_at[longest] + 1) % shape[longest]
    return array.at[tuple(index_at)].set(largest)


def level_of(rng, extent, pieces, low, high):
    def one(axis_at, blocks):
        heights = jax.random.uniform(jax.random.fold_in(jax.random.fold_in(rng, 6), axis_at), (blocks,), jnp.float32, low / len(pieces), high / len(pieces))
        return jnp.repeat(jnp.exp(heights), extent[axis_at] // blocks).reshape((-1,) + (1,) * (len(extent) - axis_at - 1))

    loudness = one(*pieces[0])
    for cut in pieces[1:]:
        loudness = loudness * one(*cut)
    return loudness


def noise(rng, dims, deviation, limit, cuts=(), kind=jnp.bfloat16):
    result = jax.random.normal(rng, dims, jnp.float32) * deviation
    if len(cuts) > 0:
        result = level_of(rng, dims, cuts, -0.22, 0.18) * result
    return jnp.clip(result, min=-limit, max=limit).astype(kind)


def setup_inputs(seed: int = 0) -> dict:
    streams_of = jax.random.split(jax.random.key(seed), 6)
    return {
        "ocean_heat_field": noise(streams_of[0], (EPOCH_TOTAL, INPUT_PATCHES, PATCH_SIDE, PATCH_SIDE), 1.0, 6.0, ((0, 8), (1, 16)), jnp.float32),
        "patch_zone": draw_patch_zone(jax.random.fold_in(streams_of[5], 71), 0),
        "patch_position": draw_patch_position(jax.random.fold_in(streams_of[5], 71), 0),
        "quarter_spins": plant(jax.random.randint(streams_of[3], (INPUT_PATCHES,), 0, 4), jax.random.fold_in(streams_of[3], 1), 0, 3).astype(jnp.int32),
        "zone_patch_tally": draw_zone_patch_tally(jax.random.fold_in(streams_of[5], 71), 0),
    }


def spin_patches(incoming_patches, turn_codes):
    first_turn = jnp.rot90(incoming_patches, 1, axes=(2, 3))
    half_turn = jnp.rot90(incoming_patches, 2, axes=(2, 3))
    last_turn = jnp.rot90(incoming_patches, 3, axes=(2, 3))
    shaped = turn_codes[None, :, None, None]
    return jnp.where(shaped == 0, incoming_patches, jnp.where(shaped == 1, first_turn, jnp.where(shaped == 2, half_turn, last_turn)))


def reference(ocean_heat_field, patch_zone, patch_position, quarter_spins, zone_patch_tally):
    spun_patches = spin_patches(ocean_heat_field, quarter_spins)
    centered = spun_patches - jnp.mean(spun_patches, axis=0, keepdims=True)
    arranged = jnp.zeros((EPOCH_TOTAL, REGIONS, CAP, PATCH_SIDE, PATCH_SIDE), jnp.float32)
    arranged = arranged.at[:, patch_zone, patch_position].set(centered)
    in_use = jnp.arange(CAP, dtype=jnp.int32)[None, :] < zone_patch_tally[:, None]
    return jnp.where(in_use[None, :, :, None, None], arranged, jnp.float32(0.0))
```

```python
import functools

import jax
import jax.numpy as jnp
from jax import lax
from jax.experimental import pallas as pl
from jax.experimental.pallas import tpu as pltpu
from jax.sharding import PartitionSpec as P

MOST = 3
AHEAD = 3


def flip_lanes(rows):
    lane = lax.broadcasted_iota(jnp.int32, rows.shape, 1)
    return jnp.take_along_axis(rows, rows.shape[1] - 1 - lane, axis=1, mode="promise_in_bounds")


def flip_rows(rows):
    row = lax.broadcasted_iota(jnp.int32, rows.shape, 0)
    return jnp.take_along_axis(rows, rows.shape[0] - 1 - row, axis=0, mode="promise_in_bounds")


def pack_kernel(region_rows, zone, spins, my_base, field, packed, turned):
    times, blocks, side, _ = field.shape
    strips = side // 8
    base = my_base[0]

    def one(j, _):
        mine = zone[base + j] // region_rows

        def count(i, seen):
            return seen + jnp.where(zone[base + i] // region_rows == mine, 1, 0)

        slot = mine * MOST + lax.fori_loop(0, j, count, 0)
        code = spins[base + j]
        for t in range(times):
            tile = field.at[t, j]

            @pl.when(code % 2 == 1)
            def _():
                turned[t] = tile[...].T

            @pl.when(code % 2 == 0)
            def _():
                turned[t] = tile[...]

            for way in range(4):

                @pl.when(code == way)
                def _():
                    for n in range(strips):
                        m = strips - 1 - n if way in (1, 2) else n
                        rows = turned[t, m * 8 : m * 8 + 8, :]
                        if way in (2, 3):
                            rows = flip_lanes(rows)
                        if way in (1, 2):
                            rows = flip_rows(rows)
                        packed[n, slot, t] = rows

        return 0

    lax.fori_loop(0, blocks, one, 0)


def exchange_kernel(
    columns, rows, pick, tally, packed, result, arrived, staged, outgoing, landed, own_sem, out_sem, xs, xr, zs, zr
):
    strips = packed.shape[0]
    times = packed.shape[2]
    capacity = landed.shape[3]
    epochs = rows * times
    column = lax.axis_index("gx")
    row = lax.axis_index("gy")

    barrier = pltpu.get_barrier_semaphore()

    def greet_column(d, _):
        pl.semaphore_signal(barrier, inc=1, device_id={"gx": lax.rem(column + d, columns)})
        return 0

    def greet_row(d, _):
        pl.semaphore_signal(barrier, inc=1, device_id={"gy": lax.rem(row + d, rows)})
        return 0

    lax.fori_loop(1, columns, greet_column, 0)
    lax.fori_loop(1, rows, greet_row, 0)
    own = pltpu.make_async_copy(
        packed.at[:, pl.ds(column * MOST, MOST)], arrived.at[:, pl.ds(column * MOST, MOST)], own_sem
    )
    own.start()
    pl.semaphore_wait(barrier, columns + rows - 2)

    def send_column(n):
        def body(d, _):
            peer = lax.rem(column + d, columns)
            pltpu.make_async_remote_copy(
                src_ref=packed.at[n, pl.ds(peer * MOST, MOST)],
                dst_ref=arrived.at[n, pl.ds(column * MOST, MOST)],
                send_sem=xs.at[n],
                recv_sem=xr.at[n],
                device_id={"gx": peer},
            ).start()
            return 0

        lax.fori_loop(1, columns, body, 0)

    def column_whole(n):
        width = (columns - 1) * MOST
        return pltpu.make_async_remote_copy(
            src_ref=packed.at[n, pl.ds(0, width)],
            dst_ref=arrived.at[n, pl.ds(0, width)],
            send_sem=xs.at[n],
            recv_sem=xr.at[n],
            device_id={"gx": lax.rem(column + 1, columns)},
        )

    def send_row(n):
        def body(d, _):
            peer = lax.rem(row + d, rows)
            pltpu.make_async_remote_copy(
                src_ref=outgoing.at[n, peer],
                dst_ref=landed.at[n, row],
                send_sem=zs.at[n],
                recv_sem=zr.at[n],
                device_id={"gy": peer},
            ).start()
            return 0

        lax.fori_loop(1, rows, body, 0)

    def row_whole(n):
        return pltpu.make_async_remote_copy(
            src_ref=outgoing.at[n, pl.ds(0, rows - 1)],
            dst_ref=landed.at[n, pl.ds(0, rows - 1)],
            send_sem=zs.at[n],
            recv_sem=zr.at[n],
            device_id={"gy": lax.rem(row + 1, rows)},
        )

    def out_copy(n):
        return pltpu.make_async_copy(
            landed.at[n], result.at[:, :, :, pl.ds(n * 8, 8), :], out_sem.at[n]
        )

    def select(n):
        for a in range(columns * MOST):
            for t in range(times):
                staged[a, t] = arrived[n, a, t]
        for r in range(rows):
            for s in range(capacity):
                source = pick[r * capacity + s]
                for t in range(times):
                    outgoing[n, r, t, s] = staged[source, t]
        for t in range(times):
            for s in range(capacity):
                landed[n, row, t, s] = staged[pick[row * capacity + s], t]

    def centre(n):
        row_whole(n).wait_recv()
        for s in range(capacity):
            total = landed[n, 0, 0, s]
            for e in range(1, epochs):
                total = total + landed[n, e // times, e % times, s]
            mean = total * jnp.float32(1.0 / epochs)
            used = s < tally[0]
            for e in range(epochs):
                value = landed[n, e // times, e % times, s]
                landed[n, e // times, e % times, s] = jnp.where(used, value - mean, 0.0)
        out_copy(n).start()

    def ahead(n, _):
        send_column(n)
        return 0

    lax.fori_loop(0, AHEAD, ahead, 0)
    own.wait()

    def step(n, _):
        column_whole(n).wait_recv()
        select(n)

        @pl.when(n + AHEAD < strips)
        def _():
            send_column(n + AHEAD)

        send_row(n)

        @pl.when(n >= 2)
        def _():
            centre(n - 2)

        return 0

    lax.fori_loop(0, strips, step, 0)
    centre(strips - 2)
    centre(strips - 1)

    def drain(n, _):
        column_whole(n).wait_send()
        row_whole(n).wait_send()
        out_copy(n).wait()
        return 0

    lax.fori_loop(0, strips, drain, 0)


def tables(patch_zone, patch_position, columns, rows, capacity):
    zone = patch_zone.reshape(columns, -1)
    column = zone // rows
    blocks = zone.shape[1]
    earlier = jnp.arange(blocks)[None, :, None] > jnp.arange(blocks)[None, None, :]
    same = column[:, :, None] == column[:, None, :]
    rank = jnp.sum(jnp.where(same & earlier, 1, 0), axis=2)
    arrival = (jnp.arange(columns)[:, None] * MOST + rank).reshape(-1)
    target = jnp.arange(rows * capacity) + lax.axis_index("gx") * (rows * capacity)
    place = patch_zone * capacity + patch_position
    return jnp.sum(jnp.where(place[None, :] == target[:, None], arrival[None, :], 0), axis=1).astype(jnp.int32)


def on_device(field, patch_zone, patch_position, spins, tally):
    times, blocks, side, _ = field.shape
    columns = lax.axis_size("gx")
    rows = lax.axis_size("gy")
    capacity = 2 * blocks // rows
    strips = side // 8
    pick = tables(patch_zone, patch_position, columns, rows, capacity)
    base = (lax.axis_index("gx") * blocks).reshape(1).astype(jnp.int32)
    smem = pl.BlockSpec(memory_space=pltpu.SMEM)
    packed = pl.pallas_call(
        functools.partial(pack_kernel, rows),
        out_shape=jax.ShapeDtypeStruct((strips, columns * MOST, times, 8, side), jnp.float32),
        in_specs=[smem, smem, smem, pl.BlockSpec(memory_space=pltpu.VMEM)],
        out_specs=pl.BlockSpec(memory_space=pltpu.VMEM),
        scratch_shapes=[pltpu.VMEM((times, side, side), jnp.float32)],
        name="pack",
    )(patch_zone, spins, base, field)
    result = pl.pallas_call(
        functools.partial(exchange_kernel, columns, rows),
        out_shape=jax.ShapeDtypeStruct((rows, times, capacity, side, side), jnp.float32),
        in_specs=[smem, smem, pl.BlockSpec(memory_space=pl.ANY)],
        out_specs=pl.BlockSpec(memory_space=pl.ANY),
        scratch_shapes=[
            pltpu.VMEM((strips, columns * MOST, times, 8, side), jnp.float32),
            pltpu.VMEM((columns * MOST, times, 8, side), jnp.float32),
            pltpu.VMEM((strips, rows, times, capacity, 8, side), jnp.float32),
            pltpu.VMEM((strips, rows, times, capacity, 8, side), jnp.float32),
            pltpu.SemaphoreType.DMA,
            pltpu.SemaphoreType.DMA((strips,)),
            pltpu.SemaphoreType.DMA((strips,)),
            pltpu.SemaphoreType.DMA((strips,)),
            pltpu.SemaphoreType.DMA((strips,)),
            pltpu.SemaphoreType.DMA((strips,)),
        ],
        compiler_params=pltpu.CompilerParams(collective_id=0, has_side_effects=True),
        name="exchange",
    )(pick, tally, packed)
    return result.reshape(rows * times, 1, capacity, side, side)


def solution(mesh):
    placed = (P("gy", "gx", None, None), P(), P(), P(), P(("gx", "gy")))
    return jax.shard_map(
        on_device,
        mesh=mesh,
        in_specs=placed,
        out_specs=P(None, ("gx", "gy"), None, None, None),
        check_vma=False,
    )
```

```python
import functools

import jax
import jax.numpy as jnp
from jax import lax
from jax.experimental import pallas as pl
from jax.experimental.pallas import tpu as pltpu
from jax.sharding import PartitionSpec as P

MOST = 3
AHEAD = 6
TURNS = 3


def gather_lanes(rows, index):
    return jnp.take_along_axis(rows, index, axis=1, mode="promise_in_bounds")


def gather_rows(rows, index):
    return jnp.take_along_axis(rows, index, axis=0, mode="promise_in_bounds")


def maybe_reversed(axis, flip):
    index = lax.broadcasted_iota(jnp.int32, (8, 128), axis)
    return jnp.where(flip, (8, 128)[axis] - 1 - index, index)


def turn(tile, code):
    strips = tile.shape[0] // 8
    cut = [tile[8 * n : 8 * n + 8] for n in range(strips)]
    odd = code % 2 == 1
    half = code == 2
    last = code == 3
    rows_back = jnp.logical_or(code == 1, half)
    lanes = maybe_reversed(1, half)
    flat = [gather_lanes(rows, lanes) for rows in cut]
    before = maybe_reversed(0, last)
    ahead = [gather_rows(jnp.where(last, cut[strips - 1 - n], cut[n]), before) for n in range(strips)]
    crossed = jnp.concatenate(ahead, axis=0).T
    taken = [jnp.where(odd, crossed[8 * n : 8 * n + 8], flat[n]) for n in range(strips)]
    after = maybe_reversed(0, rows_back)
    return [gather_rows(jnp.where(rows_back, taken[strips - 1 - n], taken[n]), after) for n in range(strips)]


def exchange_kernel(
    columns, rows, send, pick, spins, field, result,
    turned, packed, arrived, staged, outgoing, xs, xr, zs, zr,
):
    times, blocks, side, _ = field.shape
    strips = side // 8
    chunks = times * strips
    capacity = outgoing.shape[2]
    column = lax.axis_index("gx")
    row = lax.axis_index("gy")

    barrier = pltpu.get_barrier_semaphore()

    def greet_column(d, _):
        pl.semaphore_signal(barrier, inc=1, device_id={"gx": lax.rem(column + d, columns)})
        return 0

    def greet_row(d, _):
        pl.semaphore_signal(barrier, inc=1, device_id={"gy": lax.rem(row + d, rows)})
        return 0

    lax.fori_loop(1, columns, greet_column, 0)
    lax.fori_loop(1, rows, greet_row, 0)

    def turn_block(t, j):
        strips_of = turn(field[t, j], spins[column * blocks + j])
        for n in range(strips):
            turned[t, n, j] = strips_of[n]

    def turn_first(j, _):
        turn_block(0, 2 * j)
        turn_block(0, 2 * j + 1)
        return 0

    lax.fori_loop(0, blocks // 2, turn_first, 0)

    def pack(m):
        for p in range(columns * MOST):
            packed[m, p] = turned[m // strips, m % strips, send[p]]

    def send_column(m):
        def body(d, _):
            peer = lax.rem(column + d, columns)
            pltpu.make_async_remote_copy(
                src_ref=packed.at[m, pl.ds(peer * MOST, MOST)],
                dst_ref=arrived.at[m, pl.ds(column * MOST, MOST)],
                send_sem=xs.at[m],
                recv_sem=xr.at[m],
                device_id={"gx": peer},
            ).start()
            return 0

        lax.fori_loop(1, columns, body, 0)

    def column_whole(m):
        width = (columns - 1) * MOST
        return pltpu.make_async_remote_copy(
            src_ref=packed.at[m, pl.ds(0, width)],
            dst_ref=arrived.at[m, pl.ds(0, width)],
            send_sem=xs.at[m],
            recv_sem=xr.at[m],
            device_id={"gx": lax.rem(column + 1, columns)},
        )

    def landing(r, m):
        return result.at[r, m // strips, :, pl.ds((m % strips) * 8, 8), :]

    def send_row(m):
        def body(d, _):
            peer = lax.rem(row + d, rows)
            pltpu.make_async_remote_copy(
                src_ref=outgoing.at[m, peer],
                dst_ref=landing(row, m),
                send_sem=zs.at[m],
                recv_sem=zr.at[m],
                device_id={"gy": peer},
            ).start()
            return 0

        lax.fori_loop(1, rows, body, 0)

    def row_whole(m):
        return pltpu.make_async_remote_copy(
            src_ref=outgoing.at[m, pl.ds(0, rows - 1)],
            dst_ref=outgoing.at[m, pl.ds(0, rows - 1)],
            send_sem=zs.at[m],
            recv_sem=zr.at[m],
            device_id={"gy": lax.rem(row + 1, rows)},
        )

    def select(m):
        for a in range(columns * MOST):
            staged[a] = arrived[m, a]
        for q in range(MOST):
            staged[column * MOST + q] = packed[m, column * MOST + q]
        for r in range(rows):
            for s in range(capacity):
                outgoing[m, r, s] = staged[pick[r * capacity + s]]
        here = landing(row, m)
        for s in range(capacity):
            here[s] = outgoing[m, row, s]

    pl.semaphore_wait(barrier, columns + rows - 2)

    def ahead(m, _):
        pack(m)
        send_column(m)
        return 0

    lax.fori_loop(0, AHEAD, ahead, 0)

    def step(m, _):
        @pl.when(m < (times - 1) * blocks // TURNS)
        def _():
            for i in range(TURNS):
                at = m * TURNS + i
                turn_block(1 + at // blocks, at % blocks)

        @pl.when(m + AHEAD < chunks)
        def _():
            pack(m + AHEAD)

        column_whole(m).wait_recv()
        select(m)

        @pl.when(m + AHEAD < chunks)
        def _():
            send_column(m + AHEAD)

        send_row(m)
        return 0

    lax.fori_loop(0, chunks, step, 0)

    def drain(m, _):
        column_whole(m).wait_send()
        row_whole(m).wait()
        return 0

    lax.fori_loop(0, chunks, drain, 0)


def centre_kernel(tally, regional, result, centred, out_sem):
    epochs, capacity, side, _ = regional.shape

    def put(s):
        return pltpu.make_async_copy(centred.at[:, s], result.at[:, s], out_sem.at[s])

    for s in range(capacity):

        @pl.when(s < tally[0])
        def _():
            def strip(n, _):
                at = pl.ds(n * 8, 8)
                values = [regional[e, s, at, :] for e in range(epochs)]
                level = values
                while len(level) > 1:
                    level = [a + b for a, b in zip(level[::2], level[1::2])]
                mean = level[0] * jnp.float32(1.0 / epochs)
                for e in range(epochs):
                    centred[e, s, at, :] = values[e] - mean
                return 0

            lax.fori_loop(0, side // 8, strip, 0, unroll=2)

        @pl.when(s >= tally[0])
        def _():
            def strip(n, _):
                for e in range(epochs):
                    centred[e, s, pl.ds(n * 8, 8), :] = jnp.zeros((8, side), jnp.float32)
                return 0

            lax.fori_loop(0, side // 8, strip, 0, unroll=2)

        put(s).start()
    for s in range(capacity):
        put(s).wait()


def tables(patch_zone, patch_position, columns, rows, capacity):
    total = patch_zone.shape[0]
    blocks = total // columns
    me = lax.axis_index("gx")
    block = jnp.arange(total, dtype=jnp.int32)
    group = block // blocks
    key = group * columns + patch_zone // rows
    before = (key[None, :] == key[:, None]) & (block[None, :] < block[:, None])
    rank = jnp.sum(jnp.where(before, 1, 0), axis=1)
    place = patch_zone * capacity + patch_position - me * (rows * capacity)
    target = jnp.arange(rows * capacity, dtype=jnp.int32)
    pick = jnp.sum(jnp.where(place[None, :] == target[:, None], (group * MOST + rank)[None, :], 0), axis=1)
    slot = jnp.where(group == me, (patch_zone // rows) * MOST + rank, -1)
    out_slot = jnp.arange(columns * MOST, dtype=jnp.int32)
    send = jnp.sum(jnp.where(slot[None, :] == out_slot[:, None], (block - me * blocks)[None, :], 0), axis=1)
    return send.astype(jnp.int32), pick.astype(jnp.int32)


def on_device(field, patch_zone, patch_position, spins, tally):
    times, blocks, side, _ = field.shape
    columns = lax.axis_size("gx")
    rows = lax.axis_size("gy")
    capacity = 2 * blocks // rows
    strips = side // 8
    chunks = times * strips
    send, pick = tables(patch_zone, patch_position, columns, rows, capacity)
    smem = pl.BlockSpec(memory_space=pltpu.SMEM)
    vmem = pl.BlockSpec(memory_space=pltpu.VMEM)
    anywhere = pl.BlockSpec(memory_space=pl.ANY)
    arrived = pl.pallas_call(
        functools.partial(exchange_kernel, columns, rows),
        out_shape=pltpu.VMEM((rows, times, capacity, side, side), jnp.float32),
        in_specs=[smem, smem, smem, vmem],
        out_specs=vmem,
        scratch_shapes=[
            pltpu.VMEM((times, strips, blocks, 8, side), jnp.float32),
            pltpu.VMEM((chunks, columns * MOST, 8, side), jnp.float32),
            pltpu.VMEM((chunks, columns * MOST, 8, side), jnp.float32),
            pltpu.VMEM((columns * MOST, 8, side), jnp.float32),
            pltpu.VMEM((chunks, rows, capacity, 8, side), jnp.float32),
            pltpu.SemaphoreType.DMA((chunks,)),
            pltpu.SemaphoreType.DMA((chunks,)),
            pltpu.SemaphoreType.DMA((chunks,)),
            pltpu.SemaphoreType.DMA((chunks,)),
        ],
        compiler_params=pltpu.CompilerParams(
            collective_id=0, has_side_effects=True, vmem_limit_bytes=36 * 2**20
        ),
        name="exchange",
    )(send, pick, spins, pltpu.with_memory_space_constraint(field, pltpu.VMEM))
    regional = arrived.reshape(rows * times, capacity, side, side)
    centred = pl.pallas_call(
        centre_kernel,
        out_shape=jax.ShapeDtypeStruct((rows * times, capacity, side, side), jnp.float32),
        in_specs=[smem, vmem],
        out_specs=anywhere,
        scratch_shapes=[
            pltpu.VMEM((rows * times, capacity, side, side), jnp.float32),
            pltpu.SemaphoreType.DMA((capacity,)),
        ],
        compiler_params=pltpu.CompilerParams(vmem_limit_bytes=20 * 2**20),
        name="centre",
    )(tally, regional)
    return centred[:, None]


def solution(mesh):
    placed = (P("gy", "gx", None, None), P(), P(), P(), P(("gx", "gy")))
    return jax.shard_map(
        on_device,
        mesh=mesh,
        in_specs=placed,
        out_specs=P(None, ("gx", "gy"), None, None, None),
        check_vma=False,
    )
```

```python
import functools
import math

import jax
import jax.numpy as jnp
from jax import lax
from jax.experimental import pallas as pl
from jax.experimental.pallas import tpu as pltpu
from jax.sharding import PartitionSpec as P

MOST = 3
AHEAD = 6
HALF = 64
PIECES = 4
TURNS = 3


def offsets(columns):
    width = math.isqrt(columns)
    far = [min(d, width - d) for d in range(width)]
    steps = [(dx, dy) for dx in range(width) for dy in range(width) if dx or dy]
    return sorted(steps, key=lambda step: -(far[step[0]] + far[step[1]]))


def gather_lanes(rows, index):
    return jnp.take_along_axis(rows, index, axis=1, mode="promise_in_bounds")


def gather_rows(rows, index):
    return jnp.take_along_axis(rows, index, axis=0, mode="promise_in_bounds")


def maybe_reversed(axis, flip):
    index = lax.broadcasted_iota(jnp.int32, (8, 128), axis)
    return jnp.where(flip, (8, 128)[axis] - 1 - index, index)


def turn(tile, code):
    strips = tile.shape[0] // 8
    cut = [tile[8 * n : 8 * n + 8] for n in range(strips)]
    odd = code % 2 == 1
    half = code == 2
    last = code == 3
    rows_back = jnp.logical_or(code == 1, half)
    lanes = maybe_reversed(1, half)
    flat = [gather_lanes(rows, lanes) for rows in cut]
    before = maybe_reversed(0, last)
    ahead = [gather_rows(jnp.where(last, cut[strips - 1 - n], cut[n]), before) for n in range(strips)]
    crossed = jnp.concatenate(ahead, axis=0).T
    taken = [jnp.where(odd, crossed[8 * n : 8 * n + 8], flat[n]) for n in range(strips)]
    after = maybe_reversed(0, rows_back)
    return [gather_rows(jnp.where(rows_back, taken[strips - 1 - n], taken[n]), after) for n in range(strips)]


def earlier(flat, d):
    above = jnp.concatenate([flat[:1], flat[:-1]], axis=0)
    lane = lax.broadcasted_iota(jnp.int32, flat.shape, 1)
    return jnp.where(lane >= d, pltpu.roll(flat, d, 1), pltpu.roll(above, d, 1))


def tables(zone, place, columns, rows, blocks, capacity):
    me = lax.axis_index("gx")
    line = lax.broadcasted_iota(jnp.int32, zone.shape, 0) * 128 + lax.broadcasted_iota(jnp.int32, zone.shape, 1)
    group = line // blocks
    within = line - group * blocks
    column = zone // rows
    rank = jnp.zeros_like(zone)
    for d in range(1, blocks):
        rank += jnp.where((within >= d) & (earlier(column, d) == column), 1, 0)
    place = zone * capacity + place - me * (rows * capacity)
    place = jnp.where((place >= 0) & (place < rows * capacity), place, -1)
    slot = jnp.where(group == me, column * MOST + rank + HALF, -1)
    pad = jnp.full((4 - zone.shape[0], 128), -1, jnp.int32)
    both = jnp.concatenate([place, pad, slot, pad], axis=0).T
    values = jnp.concatenate([group * MOST + rank, pad, within, pad], axis=0).T
    lane = lax.broadcasted_iota(jnp.int32, (128, 128), 1)
    total = jnp.zeros((128, 128), jnp.int32)
    for i in range(zone.shape[0]):
        for k in (i, 4 + i):
            total += jnp.where(both[:, k : k + 1] == lane, values[:, k : k + 1], 0)
    found = jnp.sum(total, axis=0, keepdims=True)
    last = jnp.where(lane[:1] < HALF, columns * MOST - 1, blocks - 1)
    return jnp.minimum(found, last)


def exchange_kernel(
    columns, rows, zone, place, spins, field, result,
    zone_v, place_v, table_v, table, turns, loaded, turned, packed, arrived, staged, outgoing,
    small_sem, load_sem, xs, xr, zs, zr,
):
    times, blocks, side, _ = loaded.shape
    strips = side // 8
    chunks = times * strips
    capacity = outgoing.shape[2]
    column = lax.axis_index("gx")
    row = lax.axis_index("gy")
    third = blocks // PIECES

    small = [
        pltpu.make_async_copy(zone, zone_v, small_sem.at[0]),
        pltpu.make_async_copy(place, place_v, small_sem.at[1]),
        pltpu.make_async_copy(spins, turns, small_sem.at[2]),
    ]
    for copy in small:
        copy.start()

    def load(t, i):
        cut = pl.ds(i * third, third)
        return pltpu.make_async_copy(field.at[t, cut], loaded.at[t, cut], load_sem.at[t, i])

    for t in range(times):
        for i in range(PIECES):
            load(t, i).start()

    barrier = pltpu.get_barrier_semaphore()

    def greet_column(d, _):
        pl.semaphore_signal(barrier, inc=1, device_id={"gx": lax.rem(column + d, columns)})
        return 0

    def greet_row(d, _):
        pl.semaphore_signal(barrier, inc=1, device_id={"gy": lax.rem(row + d, rows)})
        return 0

    lax.fori_loop(1, columns, greet_column, 0)
    lax.fori_loop(1, rows, greet_row, 0)

    for copy in small:
        copy.wait()
    table_v[...] = tables(zone_v[...], place_v[...], columns, rows, blocks, capacity)
    to_scalars = pltpu.make_async_copy(table_v, table, small_sem.at[3])

    def turn_block(t, j):
        strips_of = turn(loaded[t, j], turns[column * blocks + j])
        for n in range(strips):
            turned[t, n, j] = strips_of[n]

    for i in range(PIECES):
        load(0, i).wait()
        if i == 1:
            to_scalars.start()

        def turn_first(j, _):
            turn_block(0, i * third + 2 * j)
            turn_block(0, i * third + 2 * j + 1)
            return 0

        lax.fori_loop(0, third // 2, turn_first, 0)
    for t in range(1, times):
        for i in range(PIECES):
            load(t, i).wait()
    to_scalars.wait()

    def pack(m):
        for p in range(columns * MOST):
            packed[m, p] = turned[m // strips, m % strips, table[0, HALF + p]]

    def send_column(m):
        for dx, dy in offsets(columns):
            width = math.isqrt(columns)
            peer = lax.rem(column // width + dx, width) * width + lax.rem(column % width + dy, width)
            pltpu.make_async_remote_copy(
                src_ref=packed.at[m, pl.ds(peer * MOST, MOST)],
                dst_ref=arrived.at[m, pl.ds(column * MOST, MOST)],
                send_sem=xs.at[m],
                recv_sem=xr.at[m],
                device_id={"gx": peer},
            ).start()

    def column_whole(m):
        width = (columns - 1) * MOST
        return pltpu.make_async_remote_copy(
            src_ref=packed.at[m, pl.ds(0, width)],
            dst_ref=arrived.at[m, pl.ds(0, width)],
            send_sem=xs.at[m],
            recv_sem=xr.at[m],
            device_id={"gx": lax.rem(column + 1, columns)},
        )

    def landing(r, m):
        return result.at[r, m // strips, :, pl.ds((m % strips) * 8, 8), :]

    def send_row(m):
        def body(d, _):
            peer = lax.rem(row + d, rows)
            pltpu.make_async_remote_copy(
                src_ref=outgoing.at[m, peer],
                dst_ref=landing(row, m),
                send_sem=zs.at[m],
                recv_sem=zr.at[m],
                device_id={"gy": peer},
            ).start()
            return 0

        lax.fori_loop(1, rows, body, 0)

    def row_whole(m):
        return pltpu.make_async_remote_copy(
            src_ref=outgoing.at[m, pl.ds(0, rows - 1)],
            dst_ref=outgoing.at[m, pl.ds(0, rows - 1)],
            send_sem=zs.at[m],
            recv_sem=zr.at[m],
            device_id={"gy": lax.rem(row + 1, rows)},
        )

    def select(m):
        for a in range(columns * MOST):
            staged[a] = arrived[m, a]
        for q in range(MOST):
            staged[column * MOST + q] = packed[m, column * MOST + q]
        for r in range(rows):
            for s in range(capacity):
                outgoing[m, r, s] = staged[table[0, r * capacity + s]]
        here = landing(row, m)
        for s in range(capacity):
            here[s] = outgoing[m, row, s]

    pl.semaphore_wait(barrier, columns + rows - 2)

    def ahead(m, _):
        pack(m)
        send_column(m)
        return 0

    lax.fori_loop(0, AHEAD, ahead, 0)

    def step(m, _):
        @pl.when(m < (times - 1) * blocks // TURNS)
        def _():
            for i in range(TURNS):
                at = m * TURNS + i
                turn_block(1 + at // blocks, at % blocks)

        @pl.when(m + AHEAD < chunks)
        def _():
            pack(m + AHEAD)

        column_whole(m).wait_recv()
        select(m)

        @pl.when(m + AHEAD < chunks)
        def _():
            send_column(m + AHEAD)

        send_row(m)
        return 0

    lax.fori_loop(0, chunks, step, 0)

    def drain(m, _):
        column_whole(m).wait_send()
        row_whole(m).wait()
        return 0

    lax.fori_loop(0, chunks, drain, 0)


def centre_kernel(tally, regional, result, centred, out_sem):
    epochs, capacity, side, _ = regional.shape

    def put(s):
        return pltpu.make_async_copy(centred.at[:, s], result.at[:, s], out_sem.at[s])

    for s in range(capacity):

        @pl.when(s < tally[0])
        def _():
            def strip(n, _):
                at = pl.ds(n * 8, 8)
                values = [regional[e, s, at, :] for e in range(epochs)]
                level = values
                while len(level) > 1:
                    level = [a + b for a, b in zip(level[::2], level[1::2])]
                mean = level[0] * jnp.float32(1.0 / epochs)
                for e in range(epochs):
                    centred[e, s, at, :] = values[e] - mean
                return 0

            lax.fori_loop(0, side // 8, strip, 0, unroll=2)

        @pl.when(s >= tally[0])
        def _():
            def strip(n, _):
                for e in range(epochs):
                    centred[e, s, pl.ds(n * 8, 8), :] = jnp.zeros((8, side), jnp.float32)
                return 0

            lax.fori_loop(0, side // 8, strip, 0, unroll=2)

        put(s).start()
    for s in range(capacity):
        put(s).wait()


def on_device(field, patch_zone, patch_position, spins, tally):
    times, blocks, side, _ = field.shape
    columns = lax.axis_size("gx")
    rows = lax.axis_size("gy")
    capacity = 2 * blocks // rows
    strips = side // 8
    chunks = times * strips
    smem = pl.BlockSpec(memory_space=pltpu.SMEM)
    vmem = pl.BlockSpec(memory_space=pltpu.VMEM)
    hbm = pl.BlockSpec(memory_space=pltpu.HBM)
    lines = patch_zone.shape[0] // 128
    anywhere = pl.BlockSpec(memory_space=pl.ANY)
    operands = (patch_zone.reshape(lines, 128), patch_position.reshape(lines, 128), spins, field)
    arrived = pl.pallas_call(
        functools.partial(exchange_kernel, columns, rows),
        out_shape=pltpu.VMEM((rows, times, capacity, side, side), jnp.float32),
        in_specs=[hbm, hbm, hbm, hbm],
        out_specs=vmem,
        scratch_shapes=[
            pltpu.VMEM((lines, 128), jnp.int32),
            pltpu.VMEM((lines, 128), jnp.int32),
            pltpu.VMEM((1, 128), jnp.int32),
            pltpu.SMEM((1, 128), jnp.int32),
            pltpu.SMEM(spins.shape, jnp.int32),
            pltpu.VMEM((times, blocks, side, side), jnp.float32),
            pltpu.VMEM((times, strips, blocks, 8, side), jnp.float32),
            pltpu.VMEM((chunks, columns * MOST, 8, side), jnp.float32),
            pltpu.VMEM((chunks, columns * MOST, 8, side), jnp.float32),
            pltpu.VMEM((columns * MOST, 8, side), jnp.float32),
            pltpu.VMEM((chunks, rows, capacity, 8, side), jnp.float32),
            pltpu.SemaphoreType.DMA((4,)),
            pltpu.SemaphoreType.DMA((times, PIECES)),
            pltpu.SemaphoreType.DMA((chunks,)),
            pltpu.SemaphoreType.DMA((chunks,)),
            pltpu.SemaphoreType.DMA((chunks,)),
            pltpu.SemaphoreType.DMA((chunks,)),
        ],
        compiler_params=pltpu.CompilerParams(
            collective_id=0, has_side_effects=True, vmem_limit_bytes=36 * 2**20
        ),
        name="exchange",
    )(*(pltpu.with_memory_space_constraint(a, pltpu.HBM) for a in operands))
    regional = arrived.reshape(rows * times, capacity, side, side)
    centred = pl.pallas_call(
        centre_kernel,
        out_shape=jax.ShapeDtypeStruct((rows * times, capacity, side, side), jnp.float32),
        in_specs=[smem, vmem],
        out_specs=anywhere,
        scratch_shapes=[
            pltpu.VMEM((rows * times, capacity, side, side), jnp.float32),
            pltpu.SemaphoreType.DMA((capacity,)),
        ],
        compiler_params=pltpu.CompilerParams(vmem_limit_bytes=20 * 2**20),
        name="centre",
    )(tally, regional)
    return centred[:, None]


def solution(mesh):
    placed = (P("gy", "gx", None, None), P(), P(), P(), P(("gx", "gy")))
    return jax.shard_map(
        on_device,
        mesh=mesh,
        in_specs=placed,
        out_specs=P(None, ("gx", "gy"), None, None, None),
        check_vma=False,
    )
```

```python
import functools
import math

import jax
import jax.numpy as jnp
from jax import lax
from jax.experimental import pallas as pl
from jax.experimental.pallas import tpu as pltpu
from jax.sharding import PartitionSpec as P

MOST = 3
AHEAD = 6
HALF = 64
USED = HALF - 1
LAG = 4
PIECES = 3
TURNS = 3


def offsets(columns):
    width = math.isqrt(columns)
    far = [min(d, width - d) for d in range(width)]
    steps = [(dx, dy) for dx in range(width) for dy in range(width) if dx or dy]
    return sorted(steps, key=lambda step: -(far[step[0]] + far[step[1]]))


def gather_lanes(rows, index):
    return jnp.take_along_axis(rows, index, axis=1, mode="promise_in_bounds")


def gather_rows(rows, index):
    return jnp.take_along_axis(rows, index, axis=0, mode="promise_in_bounds")


def maybe_reversed(axis, flip):
    index = lax.broadcasted_iota(jnp.int32, (8, 128), axis)
    return jnp.where(flip, (8, 128)[axis] - 1 - index, index)


def turn(tile, code):
    strips = tile.shape[0] // 8
    cut = [tile[8 * n : 8 * n + 8] for n in range(strips)]
    odd = code % 2 == 1
    half = code == 2
    last = code == 3
    rows_back = jnp.logical_or(code == 1, half)
    lanes = maybe_reversed(1, half)
    flat = [gather_lanes(rows, lanes) for rows in cut]
    before = maybe_reversed(0, last)
    ahead = [gather_rows(jnp.where(last, cut[strips - 1 - n], cut[n]), before) for n in range(strips)]
    crossed = jnp.concatenate(ahead, axis=0).T
    taken = [jnp.where(odd, crossed[8 * n : 8 * n + 8], flat[n]) for n in range(strips)]
    after = maybe_reversed(0, rows_back)
    return [gather_rows(jnp.where(rows_back, taken[strips - 1 - n], taken[n]), after) for n in range(strips)]


def earlier(flat, d):
    above = jnp.concatenate([flat[:1], flat[:-1]], axis=0)
    lane = lax.broadcasted_iota(jnp.int32, flat.shape, 1)
    return jnp.where(lane >= d, pltpu.roll(flat, d, 1), pltpu.roll(above, d, 1))


def tables(zone, place, columns, rows, blocks, capacity):
    me = lax.axis_index("gx")
    line = lax.broadcasted_iota(jnp.int32, zone.shape, 0) * 128 + lax.broadcasted_iota(jnp.int32, zone.shape, 1)
    group = line // blocks
    within = line - group * blocks
    column = zone // rows
    rank = jnp.zeros_like(zone)
    for d in range(1, blocks):
        rank += jnp.where((within >= d) & (earlier(column, d) == column), 1, 0)
    place = zone * capacity + place - me * (rows * capacity)
    place = jnp.where((place >= 0) & (place < rows * capacity), place, -1)
    slot = jnp.where(group == me, column * MOST + rank + HALF, -1)
    pad = jnp.full((4 - zone.shape[0], 128), -1, jnp.int32)
    region = me * rows + lax.axis_index("gy")
    both = jnp.concatenate([place, pad, slot, pad], axis=0).T
    ours = jnp.concatenate([jnp.where(zone == region, USED, -1), pad, pad, pad, pad, pad], axis=0).T
    values = jnp.concatenate([group * MOST + rank, pad, within, pad], axis=0).T
    lane = lax.broadcasted_iota(jnp.int32, (128, 128), 1)
    total = jnp.zeros((128, 128), jnp.int32)
    for i in range(zone.shape[0]):
        for k in (i, 4 + i):
            total += jnp.where(both[:, k : k + 1] == lane, values[:, k : k + 1], 0)
        total += jnp.where(ours[:, i : i + 1] == lane, 1, 0)
    found = jnp.sum(total, axis=0, keepdims=True)
    last = jnp.where(lane[:1] < HALF, columns * MOST - 1, blocks - 1)
    return jnp.minimum(found, last)


def exchange_kernel(
    columns, rows, zone, place, spins, field, result,
    zone_v, place_v, table_v, table, turns, loaded, turned, packed, arrived, staged, outgoing,
    small_sem, load_sem, xs, xr, zs, zr,
):
    times, blocks, side, _ = loaded.shape
    strips = side // 8
    chunks = times * strips
    capacity = outgoing.shape[2]
    column = lax.axis_index("gx")
    row = lax.axis_index("gy")
    third = blocks // PIECES

    small = [
        pltpu.make_async_copy(zone, zone_v, small_sem.at[0]),
        pltpu.make_async_copy(place, place_v, small_sem.at[1]),
        pltpu.make_async_copy(spins, turns, small_sem.at[2]),
    ]
    for copy in small:
        copy.start()

    def load(t, i):
        cut = pl.ds(i * third, third)
        return pltpu.make_async_copy(field.at[t, cut], loaded.at[t, cut], load_sem.at[t, i])

    for t in range(times):
        for i in range(PIECES):
            load(t, i).start()

    barrier = pltpu.get_barrier_semaphore()

    def greet_column(d, _):
        pl.semaphore_signal(barrier, inc=1, device_id={"gx": lax.rem(column + d, columns)})
        return 0

    def greet_row(d, _):
        pl.semaphore_signal(barrier, inc=1, device_id={"gy": lax.rem(row + d, rows)})
        return 0

    lax.fori_loop(1, columns, greet_column, 0)
    lax.fori_loop(1, rows, greet_row, 0)

    for copy in small:
        copy.wait()
    table_v[...] = tables(zone_v[...], place_v[...], columns, rows, blocks, capacity)
    to_scalars = pltpu.make_async_copy(table_v, table, small_sem.at[3])

    def turn_block(t, j):
        strips_of = turn(loaded[t, j], turns[column * blocks + j])
        for n in range(strips):
            turned[t, n, j] = strips_of[n]

    for i in range(PIECES):
        load(0, i).wait()
        if i == 1:
            to_scalars.start()

        for j in range(third):
            turn_block(0, i * third + j)
    for t in range(1, times):
        for i in range(PIECES):
            load(t, i).wait()
    to_scalars.wait()

    def pack(m):
        for p in range(columns * MOST):
            packed[m, p] = turned[m // strips, m % strips, table[0, HALF + p]]

    def send_column(m):
        for dx, dy in offsets(columns):
            width = math.isqrt(columns)
            peer = lax.rem(column // width + dx, width) * width + lax.rem(column % width + dy, width)
            pltpu.make_async_remote_copy(
                src_ref=packed.at[m, pl.ds(peer * MOST, MOST)],
                dst_ref=arrived.at[m, pl.ds(column * MOST, MOST)],
                send_sem=xs.at[m],
                recv_sem=xr.at[m],
                device_id={"gx": peer},
            ).start()

    def column_whole(m):
        width = (columns - 1) * MOST
        return pltpu.make_async_remote_copy(
            src_ref=packed.at[m, pl.ds(0, width)],
            dst_ref=arrived.at[m, pl.ds(0, width)],
            send_sem=xs.at[m],
            recv_sem=xr.at[m],
            device_id={"gx": lax.rem(column + 1, columns)},
        )

    def landing(r, m):
        return result.at[r, m // strips, :, pl.ds((m % strips) * 8, 8), :]

    def send_row(m):
        def body(d, _):
            peer = lax.rem(row + d, rows)
            pltpu.make_async_remote_copy(
                src_ref=outgoing.at[m, peer],
                dst_ref=landing(row, m),
                send_sem=zs.at[m],
                recv_sem=zr.at[m],
                device_id={"gy": peer},
            ).start()
            return 0

        lax.fori_loop(1, rows, body, 0)

    def row_whole(m):
        return pltpu.make_async_remote_copy(
            src_ref=outgoing.at[m, pl.ds(0, rows - 1)],
            dst_ref=outgoing.at[m, pl.ds(0, rows - 1)],
            send_sem=zs.at[m],
            recv_sem=zr.at[m],
            device_id={"gy": lax.rem(row + 1, rows)},
        )

    def select(m):
        for a in range(columns * MOST):
            staged[a] = arrived[m, a]
        for q in range(MOST):
            staged[column * MOST + q] = packed[m, column * MOST + q]
        for r in range(rows):
            for s in range(capacity):
                outgoing[m, r, s] = staged[table[0, r * capacity + s]]
        here = landing(row, m)
        for s in range(capacity):
            here[s] = outgoing[m, row, s]

    def centre(n):
        epochs = [(r, t) for r in range(rows) for t in range(times)]
        at = pl.ds(n * 8, 8)
        for s in range(capacity):
            values = [result[r, t, s, at, :] for r, t in epochs]
            level = values
            while len(level) > 1:
                level = [a + b for a, b in zip(level[::2], level[1::2])]
            mean = level[0] * jnp.float32(1.0 / len(epochs))
            used = s < table[0, USED]
            for (r, t), value in zip(epochs, values):
                result[r, t, s, at, :] = jnp.where(used, value - mean, 0.0)

    pl.semaphore_wait(barrier, columns + rows - 2)

    def ahead(m, _):
        pack(m)
        send_column(m)
        return 0

    lax.fori_loop(0, AHEAD, ahead, 0)

    def step(m, _):
        @pl.when(m < (times - 1) * blocks // TURNS)
        def _():
            for i in range(TURNS):
                at = m * TURNS + i
                turn_block(1 + at // blocks, at % blocks)

        @pl.when(m + AHEAD < chunks)
        def _():
            pack(m + AHEAD)

        column_whole(m).wait_recv()
        select(m)

        @pl.when(m + AHEAD < chunks)
        def _():
            send_column(m + AHEAD)

        send_row(m)

        @pl.when(m >= LAG)
        def _():
            row_whole(m - LAG).wait_recv()

        @pl.when(m >= LAG + chunks - strips)
        def _():
            centre(m - LAG - (chunks - strips))

        return 0

    lax.fori_loop(0, chunks, step, 0)

    def finish(m, _):
        row_whole(m).wait_recv()
        centre(m - (chunks - strips))
        return 0

    lax.fori_loop(chunks - LAG, chunks, finish, 0)

    def drain(m, _):
        column_whole(m).wait_send()
        row_whole(m).wait_send()
        return 0

    lax.fori_loop(0, chunks, drain, 0)


def write_kernel(regional, result, sem):
    copies = [
        pltpu.make_async_copy(regional.at[e], result.at[e], sem.at[e]) for e in range(regional.shape[0])
    ]
    for copy in copies:
        copy.start()
    for copy in copies:
        copy.wait()


def on_device(field, patch_zone, patch_position, spins, tally):
    times, blocks, side, _ = field.shape
    columns = lax.axis_size("gx")
    rows = lax.axis_size("gy")
    capacity = 2 * blocks // rows
    strips = side // 8
    chunks = times * strips
    vmem = pl.BlockSpec(memory_space=pltpu.VMEM)
    hbm = pl.BlockSpec(memory_space=pltpu.HBM)
    lines = patch_zone.shape[0] // 128
    anywhere = pl.BlockSpec(memory_space=pl.ANY)
    operands = (patch_zone.reshape(lines, 128), patch_position.reshape(lines, 128), spins, field)
    arrived = pl.pallas_call(
        functools.partial(exchange_kernel, columns, rows),
        out_shape=pltpu.VMEM((rows, times, capacity, side, side), jnp.float32),
        in_specs=[hbm, hbm, hbm, hbm],
        out_specs=vmem,
        scratch_shapes=[
            pltpu.VMEM((lines, 128), jnp.int32),
            pltpu.VMEM((lines, 128), jnp.int32),
            pltpu.VMEM((1, 128), jnp.int32),
            pltpu.SMEM((1, 128), jnp.int32),
            pltpu.SMEM(spins.shape, jnp.int32),
            pltpu.VMEM((times, blocks, side, side), jnp.float32),
            pltpu.VMEM((times, strips, blocks, 8, side), jnp.float32),
            pltpu.VMEM((chunks, columns * MOST, 8, side), jnp.float32),
            pltpu.VMEM((chunks, columns * MOST, 8, side), jnp.float32),
            pltpu.VMEM((columns * MOST, 8, side), jnp.float32),
            pltpu.VMEM((chunks, rows, capacity, 8, side), jnp.float32),
            pltpu.SemaphoreType.DMA((4,)),
            pltpu.SemaphoreType.DMA((times, PIECES)),
            pltpu.SemaphoreType.DMA((chunks,)),
            pltpu.SemaphoreType.DMA((chunks,)),
            pltpu.SemaphoreType.DMA((chunks,)),
            pltpu.SemaphoreType.DMA((chunks,)),
        ],
        compiler_params=pltpu.CompilerParams(
            collective_id=0, has_side_effects=True, vmem_limit_bytes=36 * 2**20
        ),
        name="exchange",
    )(*(pltpu.with_memory_space_constraint(a, pltpu.HBM) for a in operands))
    regional = arrived.reshape(rows * times, capacity, side, side)
    written = pl.pallas_call(
        write_kernel,
        out_shape=jax.ShapeDtypeStruct(regional.shape, jnp.float32),
        in_specs=[vmem],
        out_specs=anywhere,
        scratch_shapes=[pltpu.SemaphoreType.DMA((rows * times,))],
        compiler_params=pltpu.CompilerParams(vmem_limit_bytes=8 * 2**20),
        name="write",
    )(regional)
    return written[:, None]


def solution(mesh):
    placed = (P("gy", "gx", None, None), P(), P(), P(), P(("gx", "gy")))
    return jax.shard_map(
        on_device,
        mesh=mesh,
        in_specs=placed,
        out_specs=P(None, ("gx", "gy"), None, None, None),
        check_vma=False,
    )
```

```python
import functools
import math

import jax
import jax.numpy as jnp
from jax import lax
from jax.experimental import pallas as pl
from jax.experimental.pallas import tpu as pltpu
from jax.sharding import PartitionSpec as P

MOST = 3
AHEAD = 8
USED = 64
LAG = 6
PIECES = 3
TURNS = 3


def offsets(columns):
    width = math.isqrt(columns)
    far = [min(d, width - d) for d in range(width)]
    steps = [(dx, dy) for dx in range(width) for dy in range(width) if dx or dy]
    return sorted(steps, key=lambda step: -(far[step[0]] + far[step[1]]))


def gather_lanes(rows, index):
    return jnp.take_along_axis(rows, index, axis=1, mode="promise_in_bounds")


def gather_rows(rows, index):
    return jnp.take_along_axis(rows, index, axis=0, mode="promise_in_bounds")


def maybe_reversed(axis, flip):
    index = lax.broadcasted_iota(jnp.int32, (8, 128), axis)
    return jnp.where(flip, (8, 128)[axis] - 1 - index, index)


def turn(tile, code):
    strips = tile.shape[0] // 8
    cut = [tile[8 * n : 8 * n + 8] for n in range(strips)]
    odd = code % 2 == 1
    half = code == 2
    last = code == 3
    rows_back = jnp.logical_or(code == 1, half)
    lanes = maybe_reversed(1, half)
    flat = [gather_lanes(rows, lanes) for rows in cut]
    before = maybe_reversed(0, last)
    ahead = [gather_rows(jnp.where(last, cut[strips - 1 - n], cut[n]), before) for n in range(strips)]
    crossed = jnp.concatenate(ahead, axis=0).T
    taken = [jnp.where(odd, crossed[8 * n : 8 * n + 8], flat[n]) for n in range(strips)]
    after = maybe_reversed(0, rows_back)
    return [gather_rows(jnp.where(rows_back, taken[strips - 1 - n], taken[n]), after) for n in range(strips)]


def earlier(flat, d):
    above = jnp.concatenate([flat[:1], flat[:-1]], axis=0)
    lane = lax.broadcasted_iota(jnp.int32, flat.shape, 1)
    return jnp.where(lane >= d, pltpu.roll(flat, d, 1), pltpu.roll(above, d, 1))


def outgoing_table(zone, columns, rows, blocks):
    base = lax.axis_index("gx") * blocks
    lane = lax.broadcasted_iota(jnp.int32, (1, 128), 1)
    column = lane // MOST
    left = lane - column * MOST
    held = jnp.zeros((1, 128), jnp.int32)
    for j in range(blocks):
        at = base + j
        same = column == zone[at // 128, at % 128] // rows
        held = jnp.where(same & (left == 0), j, held)
        left = jnp.where(same, left - 1, left)
    return held


def arriving_table(zone, place, columns, rows, blocks, capacity):
    me = lax.axis_index("gx")
    region = me * rows + lax.axis_index("gy")
    line = lax.broadcasted_iota(jnp.int32, zone.shape, 0) * 128 + lax.broadcasted_iota(jnp.int32, zone.shape, 1)
    group = line // blocks
    within = line - group * blocks
    column = zone // rows
    rank = jnp.zeros_like(zone)
    for d in range(1, blocks):
        rank += jnp.where((within >= d) & (earlier(column, d) == column), 1, 0)
    place = zone * capacity + place - me * (rows * capacity)
    place = jnp.where((place >= 0) & (place < rows * capacity), place, -1)
    ours = jnp.where(zone == region, USED, -1)
    pad = jnp.full((4 - zone.shape[0], 128), -1, jnp.int32)
    both = jnp.concatenate([place, pad, ours, pad], axis=0).T
    values = jnp.concatenate([group * MOST + rank, pad, pad, pad, pad, pad], axis=0).T
    lane = lax.broadcasted_iota(jnp.int32, (128, 128), 1)
    total = jnp.zeros((128, 128), jnp.int32)
    for i in range(zone.shape[0]):
        total += jnp.where(both[:, i : i + 1] == lane, values[:, i : i + 1], 0)
        total += jnp.where(both[:, 4 + i : 5 + i] == lane, 1, 0)
    return jnp.minimum(jnp.sum(total, axis=0, keepdims=True), columns * MOST - 1)


def exchange_kernel(
    columns, rows, zone, place, spins, field, result,
    zone_v, place_v, zone_s, table_v, send, pick, turns, loaded, turned, packed, arrived, staged, outgoing,
    small_sem, load_sem, xs, xr, zs, zr,
):
    times, blocks, side, _ = loaded.shape
    strips = side // 8
    chunks = times * strips
    capacity = outgoing.shape[2]
    column = lax.axis_index("gx")
    row = lax.axis_index("gy")
    third = blocks // PIECES

    small = [
        pltpu.make_async_copy(zone, zone_s, small_sem.at[0]),
        pltpu.make_async_copy(spins, turns, small_sem.at[1]),
        pltpu.make_async_copy(zone, zone_v, small_sem.at[2]),
        pltpu.make_async_copy(place, place_v, small_sem.at[3]),
    ]
    for copy in small:
        copy.start()

    def load(t, i):
        cut = pl.ds(i * third, third)
        return pltpu.make_async_copy(field.at[t, cut], loaded.at[t, cut], load_sem.at[t, i])

    for t in range(times):
        for i in range(PIECES):
            load(t, i).start()

    barrier = pltpu.get_barrier_semaphore()

    def greet_column(d, _):
        pl.semaphore_signal(barrier, inc=1, device_id={"gx": lax.rem(column + d, columns)})
        return 0

    def greet_row(d, _):
        pl.semaphore_signal(barrier, inc=1, device_id={"gy": lax.rem(row + d, rows)})
        return 0

    lax.fori_loop(1, columns, greet_column, 0)
    lax.fori_loop(1, rows, greet_row, 0)

    for copy in small[:2]:
        copy.wait()
    table_v[0] = outgoing_table(zone_s, columns, rows, blocks)
    to_send = pltpu.make_async_copy(table_v.at[0], send, small_sem.at[4])
    to_pick = pltpu.make_async_copy(table_v.at[1], pick, small_sem.at[5])

    def turn_block(t, j):
        strips_of = turn(loaded[t, j], turns[column * blocks + j])
        for n in range(strips):
            turned[t, n, j] = strips_of[n]

    for i in range(PIECES):
        load(0, i).wait()
        if i == 1:
            to_send.start()

        for j in range(third):
            turn_block(0, i * third + j)
    to_send.wait()

    def pack(m):
        for p in range(columns * MOST):
            packed[m, p] = turned[m // strips, m % strips, send[0, p]]

    def send_column(m):
        for dx, dy in offsets(columns):
            width = math.isqrt(columns)
            peer = lax.rem(column // width + dx, width) * width + lax.rem(column % width + dy, width)
            pltpu.make_async_remote_copy(
                src_ref=packed.at[m, pl.ds(peer * MOST, MOST)],
                dst_ref=arrived.at[m, pl.ds(column * MOST, MOST)],
                send_sem=xs.at[m],
                recv_sem=xr.at[m],
                device_id={"gx": peer},
            ).start()

    def column_whole(m):
        width = (columns - 1) * MOST
        return pltpu.make_async_remote_copy(
            src_ref=packed.at[m, pl.ds(0, width)],
            dst_ref=arrived.at[m, pl.ds(0, width)],
            send_sem=xs.at[m],
            recv_sem=xr.at[m],
            device_id={"gx": lax.rem(column + 1, columns)},
        )

    def landing(r, m):
        return result.at[r, m // strips, :, pl.ds((m % strips) * 8, 8), :]

    def send_row(m):
        for d in sorted(range(1, rows), key=lambda d: -min(d, rows - d)):
            peer = lax.rem(row + d, rows)
            pltpu.make_async_remote_copy(
                src_ref=outgoing.at[m, peer],
                dst_ref=landing(row, m),
                send_sem=zs.at[m],
                recv_sem=zr.at[m],
                device_id={"gy": peer},
            ).start()

    def row_whole(m):
        return pltpu.make_async_remote_copy(
            src_ref=outgoing.at[m, pl.ds(0, rows - 1)],
            dst_ref=outgoing.at[m, pl.ds(0, rows - 1)],
            send_sem=zs.at[m],
            recv_sem=zr.at[m],
            device_id={"gy": lax.rem(row + 1, rows)},
        )

    def select(m):
        for a in range(columns * MOST):
            staged[a] = arrived[m, a]
        for q in range(MOST):
            staged[column * MOST + q] = packed[m, column * MOST + q]
        for r in range(rows):
            for s in range(capacity):
                outgoing[m, r, s] = staged[pick[0, r * capacity + s]]
        here = landing(row, m)
        for s in range(capacity):
            here[s] = outgoing[m, row, s]

    def centre(n):
        epochs = [(r, t) for r in range(rows) for t in range(times)]
        at = pl.ds(n * 8, 8)
        for s in range(capacity):
            values = [result[r, t, s, at, :] for r, t in epochs]
            level = values
            while len(level) > 1:
                level = [a + b for a, b in zip(level[::2], level[1::2])]
            mean = level[0] * jnp.float32(1.0 / len(epochs))
            used = s < pick[0, USED]
            for (r, t), value in zip(epochs, values):
                result[r, t, s, at, :] = jnp.where(used, value - mean, 0.0)

    pl.semaphore_wait(barrier, columns + rows - 2)

    def ahead(m, _):
        pack(m)
        send_column(m)
        return 0

    lax.fori_loop(0, AHEAD, ahead, 0)
    pack(AHEAD)
    for copy in small[2:]:
        copy.wait()
    table_v[1] = arriving_table(zone_v[...], place_v[...], columns, rows, blocks, capacity)
    for t in range(1, times):
        for i in range(PIECES):
            load(t, i).wait()
    to_pick.start()
    to_pick.wait()

    def step(m, _):
        column_whole(m).wait_recv()
        select(m)

        @pl.when(m + AHEAD < chunks)
        def _():
            send_column(m + AHEAD)

        send_row(m)

        @pl.when(m < (times - 1) * blocks // TURNS)
        def _():
            for i in range(TURNS):
                at = m * TURNS + i
                turn_block(1 + at // blocks, at % blocks)

        @pl.when(m + AHEAD + 1 < chunks)
        def _():
            pack(m + AHEAD + 1)

        @pl.when(m >= LAG)
        def _():
            row_whole(m - LAG).wait_recv()

        @pl.when(m >= LAG + chunks - strips)
        def _():
            centre(m - LAG - (chunks - strips))

        return 0

    lax.fori_loop(0, chunks, step, 0)

    def finish(m, _):
        row_whole(m).wait_recv()
        centre(m - (chunks - strips))
        return 0

    lax.fori_loop(chunks - LAG, chunks, finish, 0)

    def drain(m, _):
        column_whole(m).wait_send()
        row_whole(m).wait_send()
        return 0

    lax.fori_loop(0, chunks, drain, 0)


def write_kernel(regional, result, sem):
    copy = pltpu.make_async_copy(regional, result, sem)
    copy.start()
    copy.wait()


def on_device(field, patch_zone, patch_position, spins, tally):
    times, blocks, side, _ = field.shape
    columns = lax.axis_size("gx")
    rows = lax.axis_size("gy")
    capacity = 2 * blocks // rows
    strips = side // 8
    chunks = times * strips
    vmem = pl.BlockSpec(memory_space=pltpu.VMEM)
    hbm = pl.BlockSpec(memory_space=pltpu.HBM)
    lines = patch_zone.shape[0] // 128
    anywhere = pl.BlockSpec(memory_space=pl.ANY)
    operands = (patch_zone.reshape(lines, 128), patch_position.reshape(lines, 128), spins, field)
    arrived = pl.pallas_call(
        functools.partial(exchange_kernel, columns, rows),
        out_shape=pltpu.VMEM((rows, times, capacity, side, side), jnp.float32),
        in_specs=[hbm, hbm, hbm, hbm],
        out_specs=vmem,
        scratch_shapes=[
            pltpu.VMEM((lines, 128), jnp.int32),
            pltpu.VMEM((lines, 128), jnp.int32),
            pltpu.SMEM((lines, 128), jnp.int32),
            pltpu.VMEM((2, 1, 128), jnp.int32),
            pltpu.SMEM((1, 128), jnp.int32),
            pltpu.SMEM((1, 128), jnp.int32),
            pltpu.SMEM(spins.shape, jnp.int32),
            pltpu.VMEM((times, blocks, side, side), jnp.float32),
            pltpu.VMEM((times, strips, blocks, 8, side), jnp.float32),
            pltpu.VMEM((chunks, columns * MOST, 8, side), jnp.float32),
            pltpu.VMEM((chunks, columns * MOST, 8, side), jnp.float32),
            pltpu.VMEM((columns * MOST, 8, side), jnp.float32),
            pltpu.VMEM((chunks, rows, capacity, 8, side), jnp.float32),
            pltpu.SemaphoreType.DMA((6,)),
            pltpu.SemaphoreType.DMA((times, PIECES)),
            pltpu.SemaphoreType.DMA((chunks,)),
            pltpu.SemaphoreType.DMA((chunks,)),
            pltpu.SemaphoreType.DMA((chunks,)),
            pltpu.SemaphoreType.DMA((chunks,)),
        ],
        compiler_params=pltpu.CompilerParams(
            collective_id=0, has_side_effects=True, vmem_limit_bytes=36 * 2**20
        ),
        name="exchange",
    )(*(pltpu.with_memory_space_constraint(a, pltpu.HBM) for a in operands))
    regional = arrived.reshape(rows * times, capacity, side, side)
    written = pl.pallas_call(
        write_kernel,
        out_shape=jax.ShapeDtypeStruct(regional.shape, jnp.float32),
        in_specs=[vmem],
        out_specs=anywhere,
        scratch_shapes=[pltpu.SemaphoreType.DMA],
        compiler_params=pltpu.CompilerParams(vmem_limit_bytes=8 * 2**20),
        name="write",
    )(regional)
    return written[:, None]


def solution(mesh):
    placed = (P("gy", "gx", None, None), P(), P(), P(), P(("gx", "gy")))
    return jax.shard_map(
        on_device,
        mesh=mesh,
        in_specs=placed,
        out_specs=P(None, ("gx", "gy"), None, None, None),
        check_vma=False,
    )
```

```python
import functools
import math

import jax
import jax.numpy as jnp
from jax import lax
from jax.experimental import pallas as pl
from jax.experimental.pallas import tpu as pltpu
from jax.sharding import PartitionSpec as P

MOST = 3
AHEAD = 4
USED = 64
LAG = 6
PIECES = 3
TURNS = 2


def offsets(columns):
    width = math.isqrt(columns)
    far = [min(d, width - d) for d in range(width)]
    steps = [(dx, dy) for dx in range(width) for dy in range(width) if dx or dy]
    return sorted(steps, key=lambda step: -(far[step[0]] + far[step[1]]))


def gather_lanes(rows, index):
    return jnp.take_along_axis(rows, index, axis=1, mode="promise_in_bounds")


def gather_rows(rows, index):
    return jnp.take_along_axis(rows, index, axis=0, mode="promise_in_bounds")


def maybe_reversed(axis, flip):
    index = lax.broadcasted_iota(jnp.int32, (8, 128), axis)
    return jnp.where(flip, (8, 128)[axis] - 1 - index, index)


def turn(tile, code):
    strips = tile.shape[0] // 8
    cut = [tile[8 * n : 8 * n + 8] for n in range(strips)]
    odd = code % 2 == 1
    half = code == 2
    last = code == 3
    rows_back = jnp.logical_or(code == 1, half)
    lanes = maybe_reversed(1, half)
    flat = [gather_lanes(rows, lanes) for rows in cut]
    before = maybe_reversed(0, last)
    ahead = [gather_rows(jnp.where(last, cut[strips - 1 - n], cut[n]), before) for n in range(strips)]
    crossed = jnp.concatenate(ahead, axis=0).T
    taken = [jnp.where(odd, crossed[8 * n : 8 * n + 8], flat[n]) for n in range(strips)]
    after = maybe_reversed(0, rows_back)
    return [gather_rows(jnp.where(rows_back, taken[strips - 1 - n], taken[n]), after) for n in range(strips)]


def earlier(flat, d):
    above = jnp.concatenate([flat[:1], flat[:-1]], axis=0)
    lane = lax.broadcasted_iota(jnp.int32, flat.shape, 1)
    return jnp.where(lane >= d, pltpu.roll(flat, d, 1), pltpu.roll(above, d, 1))


def outgoing_table(zone, columns, rows, blocks):
    base = lax.axis_index("gx") * blocks
    lane = lax.broadcasted_iota(jnp.int32, (1, 128), 1)
    column = lane // MOST
    left = lane - column * MOST
    held = jnp.zeros((1, 128), jnp.int32)
    for j in range(blocks):
        at = base + j
        same = column == zone[at // 128, at % 128] // rows
        held = jnp.where(same & (left == 0), j, held)
        left = jnp.where(same, left - 1, left)
    return held


def arriving_table(zone, place, columns, rows, blocks, capacity):
    me = lax.axis_index("gx")
    region = me * rows + lax.axis_index("gy")
    line = lax.broadcasted_iota(jnp.int32, zone.shape, 0) * 128 + lax.broadcasted_iota(jnp.int32, zone.shape, 1)
    group = line // blocks
    within = line - group * blocks
    column = zone // rows
    rank = jnp.zeros_like(zone)
    for d in range(1, blocks):
        rank += jnp.where((within >= d) & (earlier(column, d) == column), 1, 0)
    place = zone * capacity + place - me * (rows * capacity)
    place = jnp.where((place >= 0) & (place < rows * capacity), place, -1)
    ours = jnp.where(zone == region, USED, -1)
    pad = jnp.full((4 - zone.shape[0], 128), -1, jnp.int32)
    both = jnp.concatenate([place, pad, ours, pad], axis=0).T
    values = jnp.concatenate([group * MOST + rank, pad, pad, pad, pad, pad], axis=0).T
    lane = lax.broadcasted_iota(jnp.int32, (128, 128), 1)
    total = jnp.zeros((128, 128), jnp.int32)
    for i in range(zone.shape[0]):
        total += jnp.where(both[:, i : i + 1] == lane, values[:, i : i + 1], 0)
        total += jnp.where(both[:, 4 + i : 5 + i] == lane, 1, 0)
    return jnp.minimum(jnp.sum(total, axis=0, keepdims=True), columns * MOST - 1)


def exchange_kernel(
    columns, rows, zone, place, spins, field, result,
    zone_v, place_v, zone_s, table_v, send, pick, turns, loaded, turned, packed, arrived, staged, outgoing,
    small_sem, load_sem, xs, xr, zs, zr,
):
    times, blocks, side, _ = loaded.shape
    strips = side // 8
    chunks = times * strips
    capacity = outgoing.shape[2]
    column = lax.axis_index("gx")
    row = lax.axis_index("gy")
    third = blocks // PIECES

    small = [
        pltpu.make_async_copy(zone, zone_s, small_sem.at[0]),
        pltpu.make_async_copy(spins, turns, small_sem.at[1]),
        pltpu.make_async_copy(zone, zone_v, small_sem.at[2]),
        pltpu.make_async_copy(place, place_v, small_sem.at[3]),
    ]
    for copy in small:
        copy.start()

    def load(t, i):
        cut = pl.ds(i * third, third)
        return pltpu.make_async_copy(field.at[t, cut], loaded.at[t, cut], load_sem.at[t, i])

    for t in range(times):
        for i in range(PIECES):
            load(t, i).start()

    barrier = pltpu.get_barrier_semaphore()

    def greet_column(d, _):
        pl.semaphore_signal(barrier, inc=1, device_id={"gx": lax.rem(column + d, columns)})
        return 0

    def greet_row(d, _):
        pl.semaphore_signal(barrier, inc=1, device_id={"gy": lax.rem(row + d, rows)})
        return 0

    lax.fori_loop(1, columns, greet_column, 0)
    lax.fori_loop(1, rows, greet_row, 0)

    for copy in small[:2]:
        copy.wait()
    table_v[0] = outgoing_table(zone_s, columns, rows, blocks)
    to_send = pltpu.make_async_copy(table_v.at[0], send, small_sem.at[4])
    to_pick = pltpu.make_async_copy(table_v.at[1], pick, small_sem.at[5])

    def turn_block(t, j):
        strips_of = turn(loaded[t, j], turns[column * blocks + j])
        for n in range(strips):
            turned[t, n, j] = strips_of[n]

    for i in range(PIECES):
        load(0, i).wait()
        if i == 1:
            to_send.start()

        for j in range(third):
            turn_block(0, i * third + j)
    to_send.wait()

    def pack(m):
        for p in range(columns * MOST):
            packed[m, p] = turned[m // strips, m % strips, send[0, p]]

    core = lax.rem(row, 2)

    def send_column(m):
        for dx, dy in offsets(columns):
            width = math.isqrt(columns)
            across, down = core * dx + (1 - core) * dy, core * dy + (1 - core) * dx
            peer = lax.rem(column // width + across, width) * width + lax.rem(column % width + down, width)
            pltpu.make_async_remote_copy(
                src_ref=packed.at[m, pl.ds(peer * MOST, MOST)],
                dst_ref=arrived.at[m, pl.ds(column * MOST, MOST)],
                send_sem=xs.at[m],
                recv_sem=xr.at[m],
                device_id={"gx": peer},
            ).start()

    def column_whole(m):
        width = (columns - 1) * MOST
        return pltpu.make_async_remote_copy(
            src_ref=packed.at[m, pl.ds(0, width)],
            dst_ref=arrived.at[m, pl.ds(0, width)],
            send_sem=xs.at[m],
            recv_sem=xr.at[m],
            device_id={"gx": lax.rem(column + 1, columns)},
        )

    def landing(r, m):
        return result.at[r, m // strips, :, pl.ds((m % strips) * 8, 8), :]

    def send_row(m):
        for d in sorted(range(1, rows), key=lambda d: -min(d, rows - d)):
            peer = lax.rem(row + d, rows)
            pltpu.make_async_remote_copy(
                src_ref=outgoing.at[m, peer],
                dst_ref=landing(row, m),
                send_sem=zs.at[m],
                recv_sem=zr.at[m],
                device_id={"gy": peer},
            ).start()

    def row_whole(m):
        return pltpu.make_async_remote_copy(
            src_ref=outgoing.at[m, pl.ds(0, rows - 1)],
            dst_ref=outgoing.at[m, pl.ds(0, rows - 1)],
            send_sem=zs.at[m],
            recv_sem=zr.at[m],
            device_id={"gy": lax.rem(row + 1, rows)},
        )

    def select(m):
        for a in range(columns * MOST):
            staged[a] = arrived[m, a]
        for q in range(MOST):
            staged[column * MOST + q] = packed[m, column * MOST + q]
        for r in range(rows):
            for s in range(capacity):
                outgoing[m, r, s] = staged[pick[0, r * capacity + s]]
        here = landing(row, m)
        for s in range(capacity):
            here[s] = outgoing[m, row, s]

    def centre(n):
        epochs = [(r, t) for r in range(rows) for t in range(times)]
        at = pl.ds(n * 8, 8)
        for s in range(capacity):
            values = [result[r, t, s, at, :] for r, t in epochs]
            level = values
            while len(level) > 1:
                level = [a + b for a, b in zip(level[::2], level[1::2])]
            mean = level[0] * jnp.float32(1.0 / len(epochs))
            used = s < pick[0, USED]
            for (r, t), value in zip(epochs, values):
                result[r, t, s, at, :] = jnp.where(used, value - mean, 0.0)

    pl.semaphore_wait(barrier, columns + rows - 2)

    def ahead(m, _):
        pack(m)
        send_column(m)
        return 0

    lax.fori_loop(0, AHEAD, ahead, 0)
    pack(AHEAD)
    for copy in small[2:]:
        copy.wait()
    table_v[1] = arriving_table(zone_v[...], place_v[...], columns, rows, blocks, capacity)
    for t in range(1, times):
        for i in range(PIECES):
            load(t, i).wait()
    to_pick.start()
    to_pick.wait()

    def step(m, _):
        column_whole(m).wait_recv()
        select(m)

        @pl.when(m + AHEAD < chunks)
        def _():
            send_column(m + AHEAD)

        send_row(m)

        @pl.when(m < (times - 1) * blocks // TURNS)
        def _():
            for i in range(TURNS):
                at = m * TURNS + i
                turn_block(1 + at // blocks, at % blocks)

        @pl.when(m + AHEAD + 1 < chunks)
        def _():
            pack(m + AHEAD + 1)

        @pl.when(m >= LAG)
        def _():
            row_whole(m - LAG).wait_recv()

        @pl.when(m >= LAG + chunks - strips)
        def _():
            centre(m - LAG - (chunks - strips))

        return 0

    lax.fori_loop(0, chunks, step, 0)

    def drain(m, _):
        column_whole(m).wait_send()
        row_whole(m).wait_send()
        return 0

    lax.fori_loop(0, chunks - LAG, drain, 0)

    def finish(m, _):
        column_whole(m).wait_send()
        row_whole(m).wait_send()
        row_whole(m).wait_recv()
        centre(m - (chunks - strips))
        return 0

    lax.fori_loop(chunks - LAG, chunks, finish, 0)


def write_kernel(regional, result, sem):
    copy = pltpu.make_async_copy(regional, result, sem)
    copy.start()
    copy.wait()


def on_device(field, patch_zone, patch_position, spins, tally):
    times, blocks, side, _ = field.shape
    columns = lax.axis_size("gx")
    rows = lax.axis_size("gy")
    capacity = 2 * blocks // rows
    strips = side // 8
    chunks = times * strips
    vmem = pl.BlockSpec(memory_space=pltpu.VMEM)
    hbm = pl.BlockSpec(memory_space=pltpu.HBM)
    lines = patch_zone.shape[0] // 128
    anywhere = pl.BlockSpec(memory_space=pl.ANY)
    operands = (patch_zone.reshape(lines, 128), patch_position.reshape(lines, 128), spins, field)
    arrived = pl.pallas_call(
        functools.partial(exchange_kernel, columns, rows),
        out_shape=pltpu.VMEM((rows, times, capacity, side, side), jnp.float32),
        in_specs=[hbm, hbm, hbm, hbm],
        out_specs=vmem,
        scratch_shapes=[
            pltpu.VMEM((lines, 128), jnp.int32),
            pltpu.VMEM((lines, 128), jnp.int32),
            pltpu.SMEM((lines, 128), jnp.int32),
            pltpu.VMEM((2, 1, 128), jnp.int32),
            pltpu.SMEM((1, 128), jnp.int32),
            pltpu.SMEM((1, 128), jnp.int32),
            pltpu.SMEM(spins.shape, jnp.int32),
            pltpu.VMEM((times, blocks, side, side), jnp.float32),
            pltpu.VMEM((times, strips, blocks, 8, side), jnp.float32),
            pltpu.VMEM((chunks, columns * MOST, 8, side), jnp.float32),
            pltpu.VMEM((chunks, columns * MOST, 8, side), jnp.float32),
            pltpu.VMEM((columns * MOST, 8, side), jnp.float32),
            pltpu.VMEM((chunks, rows, capacity, 8, side), jnp.float32),
            pltpu.SemaphoreType.DMA((6,)),
            pltpu.SemaphoreType.DMA((times, PIECES)),
            pltpu.SemaphoreType.DMA((chunks,)),
            pltpu.SemaphoreType.DMA((chunks,)),
            pltpu.SemaphoreType.DMA((chunks,)),
            pltpu.SemaphoreType.DMA((chunks,)),
        ],
        compiler_params=pltpu.CompilerParams(
            collective_id=0, has_side_effects=True, vmem_limit_bytes=36 * 2**20
        ),
        name="exchange",
    )(*(pltpu.with_memory_space_constraint(a, pltpu.HBM) for a in operands))
    regional = arrived.reshape(rows * times, capacity, side, side)
    written = pl.pallas_call(
        write_kernel,
        out_shape=jax.ShapeDtypeStruct(regional.shape, jnp.float32),
        in_specs=[vmem],
        out_specs=anywhere,
        scratch_shapes=[pltpu.SemaphoreType.DMA],
        compiler_params=pltpu.CompilerParams(vmem_limit_bytes=8 * 2**20),
        name="write",
    )(regional)
    return written[:, None]


def solution(mesh):
    placed = (P("gy", "gx", None, None), P(), P(), P(), P(("gx", "gy")))
    return jax.shard_map(
        on_device,
        mesh=mesh,
        in_specs=placed,
        out_specs=P(None, ("gx", "gy"), None, None, None),
        check_vma=False,
    )
```

```python
import functools
import math

import jax
import jax.numpy as jnp
from jax import lax
from jax.experimental import pallas as pl
from jax.experimental.pallas import tpu as pltpu
from jax.sharding import PartitionSpec as P

MOST = 3
AHEAD = 4
USED = 64
LAG = 6
PIECES = 2
TURNS = 2


def offsets(columns):
    width = math.isqrt(columns)
    far = [min(d, width - d) for d in range(width)]
    steps = [(dx, dy) for dx in range(width) for dy in range(width) if dx or dy]
    return sorted(steps, key=lambda step: -(far[step[0]] + far[step[1]]))


def gather_lanes(rows, index):
    return jnp.take_along_axis(rows, index, axis=1, mode="promise_in_bounds")


def gather_rows(rows, index):
    return jnp.take_along_axis(rows, index, axis=0, mode="promise_in_bounds")


def maybe_reversed(axis, flip):
    index = lax.broadcasted_iota(jnp.int32, (8, 128), axis)
    return jnp.where(flip, (8, 128)[axis] - 1 - index, index)


def turn(tile, code):
    strips = tile.shape[0] // 8
    cut = [tile[8 * n : 8 * n + 8] for n in range(strips)]
    odd = code % 2 == 1
    half = code == 2
    last = code == 3
    rows_back = jnp.logical_or(code == 1, half)
    lanes = maybe_reversed(1, half)
    flat = [gather_lanes(rows, lanes) for rows in cut]
    before = maybe_reversed(0, last)
    ahead = [gather_rows(jnp.where(last, cut[strips - 1 - n], cut[n]), before) for n in range(strips)]
    crossed = jnp.concatenate(ahead, axis=0).T
    taken = [jnp.where(odd, crossed[8 * n : 8 * n + 8], flat[n]) for n in range(strips)]
    after = maybe_reversed(0, rows_back)
    return [gather_rows(jnp.where(rows_back, taken[strips - 1 - n], taken[n]), after) for n in range(strips)]


def earlier(flat, d):
    above = jnp.concatenate([flat[:1], flat[:-1]], axis=0)
    lane = lax.broadcasted_iota(jnp.int32, flat.shape, 1)
    return jnp.where(lane >= d, pltpu.roll(flat, d, 1), pltpu.roll(above, d, 1))


def outgoing_table(zone, columns, rows, blocks):
    base = lax.axis_index("gx") * blocks
    lane = lax.broadcasted_iota(jnp.int32, (1, 128), 1)
    column = lane // MOST
    left = lane - column * MOST
    held = jnp.zeros((1, 128), jnp.int32)
    for j in range(blocks):
        at = base + j
        same = column == zone[at // 128, at % 128] // rows
        held = jnp.where(same & (left == 0), j, held)
        left = jnp.where(same, left - 1, left)
    return held


def arriving_table(zone, place, columns, rows, blocks, capacity):
    me = lax.axis_index("gx")
    region = me * rows + lax.axis_index("gy")
    line = lax.broadcasted_iota(jnp.int32, zone.shape, 0) * 128 + lax.broadcasted_iota(jnp.int32, zone.shape, 1)
    group = line // blocks
    within = line - group * blocks
    column = zone // rows
    rank = jnp.zeros_like(zone)
    for d in range(1, blocks):
        rank += jnp.where((within >= d) & (earlier(column, d) == column), 1, 0)
    place = zone * capacity + place - me * (rows * capacity)
    place = jnp.where((place >= 0) & (place < rows * capacity), place, -1)
    ours = jnp.where(zone == region, USED, -1)
    pad = jnp.full((4 - zone.shape[0], 128), -1, jnp.int32)
    both = jnp.concatenate([place, pad, ours, pad], axis=0).T
    values = jnp.concatenate([group * MOST + rank, pad, pad, pad, pad, pad], axis=0).T
    lane = lax.broadcasted_iota(jnp.int32, (128, 128), 1)
    total = jnp.zeros((128, 128), jnp.int32)
    for i in range(zone.shape[0]):
        total += jnp.where(both[:, i : i + 1] == lane, values[:, i : i + 1], 0)
        total += jnp.where(both[:, 4 + i : 5 + i] == lane, 1, 0)
    return jnp.minimum(jnp.sum(total, axis=0, keepdims=True), columns * MOST - 1)


def exchange_kernel(
    columns, rows, zone, place, spins, field, result,
    zone_v, place_v, zone_s, table_v, send, pick, turns, loaded, turned, packed, arrived, staged, outgoing,
    small_sem, load_sem, xs, xr, zs, zr,
):
    times, blocks, side, _ = loaded.shape
    strips = side // 8
    chunks = times * strips
    capacity = outgoing.shape[2]
    column = lax.axis_index("gx")
    row = lax.axis_index("gy")
    part = blocks // PIECES

    small = [
        pltpu.make_async_copy(zone, zone_s, small_sem.at[0]),
        pltpu.make_async_copy(spins, turns, small_sem.at[1]),
        pltpu.make_async_copy(zone, zone_v, small_sem.at[2]),
        pltpu.make_async_copy(place, place_v, small_sem.at[3]),
    ]
    for copy in small:
        copy.start()

    def load(t, i):
        cut = pl.ds(i * part, part)
        return pltpu.make_async_copy(field.at[t, cut], loaded.at[t, cut], load_sem.at[t, i])

    for t in range(times):
        for i in range(PIECES):
            load(t, i).start()

    barrier = pltpu.get_barrier_semaphore()

    def greet_column(d, _):
        pl.semaphore_signal(barrier, inc=1, device_id={"gx": lax.rem(column + d, columns)})
        return 0

    def greet_row(d, _):
        pl.semaphore_signal(barrier, inc=1, device_id={"gy": lax.rem(row + d, rows)})
        return 0

    lax.fori_loop(1, columns, greet_column, 0)
    lax.fori_loop(1, rows, greet_row, 0)

    for copy in small[:2]:
        copy.wait()
    table_v[0] = outgoing_table(zone_s, columns, rows, blocks)
    to_send = pltpu.make_async_copy(table_v.at[0], send, small_sem.at[4])
    to_pick = pltpu.make_async_copy(table_v.at[1], pick, small_sem.at[5])

    def turn_block(t, j):
        strips_of = turn(loaded[t, j], turns[column * blocks + j])
        for n in range(strips):
            turned[t, n, j] = strips_of[n]

    def turn_piece(i, _):
        load(0, i).wait()

        @pl.when(i == 1)
        def _():
            to_send.start()

        for j in range(part):
            turn_block(0, i * part + j)
        return 0

    lax.fori_loop(0, PIECES, turn_piece, 0)
    to_send.wait()

    def pack(m):
        for p in range(columns * MOST):
            packed[m, p] = turned[m // strips, m % strips, send[0, p]]

    core = lax.rem(row, 2)

    def send_column(m):
        for dx, dy in offsets(columns):
            width = math.isqrt(columns)
            across, down = core * dx + (1 - core) * dy, core * dy + (1 - core) * dx
            peer = lax.rem(column // width + across, width) * width + lax.rem(column % width + down, width)
            pltpu.make_async_remote_copy(
                src_ref=packed.at[m, pl.ds(peer * MOST, MOST)],
                dst_ref=arrived.at[m, pl.ds(column * MOST, MOST)],
                send_sem=xs.at[m],
                recv_sem=xr.at[m],
                device_id={"gx": peer},
            ).start()

    def column_whole(m):
        width = (columns - 1) * MOST
        return pltpu.make_async_remote_copy(
            src_ref=packed.at[m, pl.ds(0, width)],
            dst_ref=arrived.at[m, pl.ds(0, width)],
            send_sem=xs.at[m],
            recv_sem=xr.at[m],
            device_id={"gx": lax.rem(column + 1, columns)},
        )

    def landing(r, m):
        return result.at[r, m // strips, :, pl.ds((m % strips) * 8, 8), :]

    def send_row(m, peer):
        pltpu.make_async_remote_copy(
            src_ref=outgoing.at[m, peer],
            dst_ref=landing(row, m),
            send_sem=zs.at[m],
            recv_sem=zr.at[m],
            device_id={"gy": peer},
        ).start()

    def row_whole(m):
        return pltpu.make_async_remote_copy(
            src_ref=outgoing.at[m, pl.ds(0, rows - 1)],
            dst_ref=outgoing.at[m, pl.ds(0, rows - 1)],
            send_sem=zs.at[m],
            recv_sem=zr.at[m],
            device_id={"gy": lax.rem(row + 1, rows)},
        )

    def select(m):
        for a in range(columns * MOST):
            staged[a] = arrived[m, a]
        for q in range(MOST):
            staged[column * MOST + q] = packed[m, column * MOST + q]
        waiting = None
        for d in sorted(range(1, rows), key=lambda d: -min(d, rows - d)):
            peer = lax.rem(row + d, rows)
            for s in range(capacity):
                outgoing[m, peer, s] = staged[pick[0, peer * capacity + s]]
            if waiting is not None:
                send_row(m, waiting)
            waiting = peer
        here = landing(row, m)
        for s in range(capacity):
            here[s] = staged[pick[0, row * capacity + s]]
        send_row(m, waiting)

    def centre(n):
        epochs = [(r, t) for r in range(rows) for t in range(times)]
        at = pl.ds(n * 8, 8)
        for s in range(capacity):
            values = [result[r, t, s, at, :] for r, t in epochs]
            level = values
            while len(level) > 1:
                level = [a + b for a, b in zip(level[::2], level[1::2])]
            mean = level[0] * jnp.float32(1.0 / len(epochs))
            used = s < pick[0, USED]
            for (r, t), value in zip(epochs, values):
                result[r, t, s, at, :] = jnp.where(used, value - mean, 0.0)

    pl.semaphore_wait(barrier, columns + rows - 2)

    def ahead(m, _):
        pack(m)
        send_column(m)
        return 0

    lax.fori_loop(0, AHEAD, ahead, 0)
    pack(AHEAD)
    for copy in small[2:]:
        copy.wait()
    table_v[1] = arriving_table(zone_v[...], place_v[...], columns, rows, blocks, capacity)
    for t in range(1, times):
        for i in range(PIECES):
            load(t, i).wait()
    to_pick.start()
    to_pick.wait()

    def step(m, _):
        column_whole(m).wait_recv()
        select(m)

        @pl.when(m + AHEAD < chunks)
        def _():
            send_column(m + AHEAD)

        @pl.when(m < (times - 1) * blocks // TURNS)
        def _():
            for i in range(TURNS):
                at = m * TURNS + i
                turn_block(1 + at // blocks, at % blocks)

        @pl.when(m + AHEAD + 1 < chunks)
        def _():
            pack(m + AHEAD + 1)

        @pl.when(m >= LAG)
        def _():
            row_whole(m - LAG).wait_recv()

        @pl.when(m >= LAG + chunks - strips)
        def _():
            centre(m - LAG - (chunks - strips))

        return 0

    lax.fori_loop(0, chunks, step, 0)

    def drain(m, _):
        column_whole(m).wait_send()
        row_whole(m).wait_send()
        return 0

    lax.fori_loop(0, chunks - LAG, drain, 0)

    def finish(m, _):
        column_whole(m).wait_send()
        row_whole(m).wait_send()
        row_whole(m).wait_recv()
        centre(m - (chunks - strips))
        return 0

    lax.fori_loop(chunks - LAG, chunks, finish, 0)


def write_kernel(regional, result, sem):
    copy = pltpu.make_async_copy(regional, result, sem)
    copy.start()
    copy.wait()


def on_device(field, patch_zone, patch_position, spins, tally):
    times, blocks, side, _ = field.shape
    columns = lax.axis_size("gx")
    rows = lax.axis_size("gy")
    capacity = 2 * blocks // rows
    strips = side // 8
    chunks = times * strips
    vmem = pl.BlockSpec(memory_space=pltpu.VMEM)
    hbm = pl.BlockSpec(memory_space=pltpu.HBM)
    lines = patch_zone.shape[0] // 128
    anywhere = pl.BlockSpec(memory_space=pl.ANY)
    operands = (patch_zone.reshape(lines, 128), patch_position.reshape(lines, 128), spins, field)
    arrived = pl.pallas_call(
        functools.partial(exchange_kernel, columns, rows),
        out_shape=pltpu.VMEM((rows, times, capacity, side, side), jnp.float32),
        in_specs=[hbm, hbm, hbm, hbm],
        out_specs=vmem,
        scratch_shapes=[
            pltpu.VMEM((lines, 128), jnp.int32),
            pltpu.VMEM((lines, 128), jnp.int32),
            pltpu.SMEM((lines, 128), jnp.int32),
            pltpu.VMEM((2, 1, 128), jnp.int32),
            pltpu.SMEM((1, 128), jnp.int32),
            pltpu.SMEM((1, 128), jnp.int32),
            pltpu.SMEM(spins.shape, jnp.int32),
            pltpu.VMEM((times, blocks, side, side), jnp.float32),
            pltpu.VMEM((times, strips, blocks, 8, side), jnp.float32),
            pltpu.VMEM((chunks, columns * MOST, 8, side), jnp.float32),
            pltpu.VMEM((chunks, columns * MOST, 8, side), jnp.float32),
            pltpu.VMEM((columns * MOST, 8, side), jnp.float32),
            pltpu.VMEM((chunks, rows, capacity, 8, side), jnp.float32),
            pltpu.SemaphoreType.DMA((6,)),
            pltpu.SemaphoreType.DMA((times, PIECES)),
            pltpu.SemaphoreType.DMA((chunks,)),
            pltpu.SemaphoreType.DMA((chunks,)),
            pltpu.SemaphoreType.DMA((chunks,)),
            pltpu.SemaphoreType.DMA((chunks,)),
        ],
        compiler_params=pltpu.CompilerParams(
            collective_id=0, has_side_effects=True, vmem_limit_bytes=36 * 2**20
        ),
        name="exchange",
    )(*(pltpu.with_memory_space_constraint(a, pltpu.HBM) for a in operands))
    regional = arrived.reshape(rows * times, capacity, side, side)
    written = pl.pallas_call(
        write_kernel,
        out_shape=jax.ShapeDtypeStruct(regional.shape, jnp.float32),
        in_specs=[vmem],
        out_specs=anywhere,
        scratch_shapes=[pltpu.SemaphoreType.DMA],
        compiler_params=pltpu.CompilerParams(vmem_limit_bytes=8 * 2**20),
        name="write",
    )(regional)
    return written[:, None]


def solution(mesh):
    placed = (P("gy", "gx", None, None), P(), P(), P(), P(("gx", "gy")))
    return jax.shard_map(
        on_device,
        mesh=mesh,
        in_specs=placed,
        out_specs=P(None, ("gx", "gy"), None, None, None),
        check_vma=False,
    )
```
